32 devices in a mesh: dp: 8 (over z, x), parity: 4 (over y, core).
Axes of the slice: x: 2, y: 2, z: 4, core: 2. Of those that a mesh axis runs over, the one named last changes fastest.
Arguments:
- first_moment: float32 [16384, 512], P(('dp', 'parity')), may hold values from -6 to 6
- second_moment: float32 [16384, 512], P(('dp', 'parity')), may hold values from 0.01 to 4
- new_owner: int32 [16384, 1], P(('dp', 'parity')), may hold values from 0 to 7; in each aligned block of 512 rows (0 to 511, 512 to 1023, ...) at most 80 rows name the same one
- code_index: int32 [2, 4], replicated, may hold values from 0 to 7
Outputs:
- new_first: float32 [20480, 512], P(('dp', 'parity'))
- new_second: float32 [20480, 512], P(('dp', 'parity'))
- parity: float32 [5120, 2048], P(('dp', 'parity'))
- loads: int32 [8, 4], P('dp', 'parity')
The draws below stay inside these ranges and needn't reach their ends.
Inputs may be any that keep to these rules, and one draw needn't show every extreme that they name: `new_owner`: in the rows of one device (aligned blocks of 512 rows) no owner is named more than 80 times, a bound that some owner reaches in some blocks.
All inputs are finite; a program needn't handle non-finite values.
Results may differ from the reference program's by a relative error of at most 0.0003.
Values sent between devices are 32-bit elements; how exact they have to be, the bound alone decides.
A program may use at most 64 MiB of HBM per device.

```python
import math
import jax
import jax.numpy as jnp
import numpy as np
from jax import lax

BLOCK = 512
PARITY_UNITS = 2
BLK_DEV = 512
MOST = 80
CAP = 640
BLOCKS = 16384
N_DP = 8
N_PARITY = 4


def place_ends(drawn, key, smallest, top_value):
    spot = [jax.random.randint(jax.random.fold_in(key, axis), (), 0, length) for axis, length in enumerate(drawn.shape)]
    widest = drawn.shape.index(max(drawn.shape))
    beside = spot[:widest] + [(spot[widest] + 1) % drawn.shape[widest]] + spot[widest + 1:]
    return drawn.at[tuple(spot)].set(smallest).at[tuple(beside)].set(top_value)


def block_levels(own_key, extent, split, low, high):
    level, own = 1.0, jax.random.fold_in(own_key, 6)
    for position, parts in split:
        draws = jnp.exp(jax.random.uniform(jax.random.fold_in(own, position), (parts,), jnp.float32, low / len(split), high / len(split)))
        level = level * jnp.repeat(draws, extent[position] // parts).reshape([-1 if axis == position else 1 for axis in range(len(extent))])
    return level


def shared_out(own_key, own, number, rows, number_of, top, bound, slope):
    sequence = jax.random.permutation(own_key, number_of)
    crowded, ordinary = shares(number_of, rows * top, bound, slope, True), shares(number_of, rows * top, bound, slope, False)
    places = jnp.arange(number_of)

    def named(lengths, offset_by):
        used = int((lengths > 0).sum())
        fixed = max(1, used // 4)
        passed = fixed + (places - fixed + offset_by * (used - fixed)) % max(1, number_of - fixed)
        return jnp.zeros((number_of,), jnp.int32).at[sequence[jnp.where(places < fixed, places, passed)]].set(jnp.asarray(lengths, jnp.int32))

    lengths = jnp.where(number % 4 == 0, named(crowded, number // 4), named(ordinary, number - number // 4 - 1))
    mixed = jax.random.permutation(jax.random.fold_in(own, 3), number_of)
    source_of, taker = mixed[0:number_of // 2 * 2:2], mixed[1:number_of // 2 * 2:2]
    slack = jnp.minimum(lengths[source_of] - 1, bound - lengths[taker]) // 2
    slack = jnp.where((source_of == sequence[0]) | (taker == sequence[0]) | (lengths[taker] == 0), 0, jnp.maximum(slack, 0))
    passed = jax.random.randint(jax.random.fold_in(own, 4), (number_of // 2,), 0, 1 << 20) % (slack + 1)
    lengths = lengths.at[source_of].add(-passed).at[taker].add(passed)
    items = jnp.searchsorted(jnp.cumsum(lengths), jnp.arange(rows * top), side="right").astype(jnp.int32)
    grid = items.reshape(top, rows).T
    grid = grid[jax.random.permutation(jax.random.fold_in(own, 1), rows)]
    offset_by = jax.random.randint(jax.random.fold_in(own, 2), (rows, 1), 0, top)
    return jnp.take_along_axis(grid, (jnp.arange(top)[None, :] + offset_by) % top, axis=1)


def shares(count, total, bound, skew, full):
    weights = [(1 << 20) // math.isqrt(standing ** skew) + 1 for standing in range(1, count + 1)]
    largest = bound if full else min(bound, max(-(-total // count), total * weights[0] // sum(weights)))
    least = 1 if total - largest >= count - 1 else 0
    counts, rest = [largest] + [least] * (count - 1), total - largest - least * (count - 1)
    while rest > 0:
        candidates = [i for i in range(1, count) if counts[i] < largest] or [i for i in range(1, count) if counts[i] < bound]
        mass, budget = sum([weights[i] for i in candidates]), rest
        for i in candidates:
            addition = min(bound - counts[i], max(1, budget * weights[i] // mass), rest)
            counts[i] = counts[i] + addition
            rest = rest - addition
    return np.array(counts)


def bell_draw(stream_key, extent, scale, most, pieces=(), kind=jnp.bfloat16):
    gain = block_levels(stream_key, extent, pieces, -0.22, 0.18) if pieces else 1.0
    result = jax.random.normal(stream_key, extent, jnp.float32) * scale * gain
    return jnp.minimum(jnp.maximum(result, -most), most).astype(kind)


def setup_inputs(seed: int = 0) -> dict:
    keys = jax.random.split(jax.random.key(seed), 5)
    first_moment = bell_draw(keys[0], (BLOCKS, BLOCK), 1.0, 6.0, ((0, 32),), jnp.float32)
    second_moment = jnp.clip(jnp.exp(math.log(4.0) - 5.9914646 * jax.random.uniform(keys[1], (BLOCKS, BLOCK), jnp.float32) ** block_levels(keys[1], (BLOCKS, BLOCK), ((0, 32),), -0.2, 0.2)), 0.01, 4.0)
    new_owner_keys = jax.random.split(jax.random.fold_in(keys[2], 1), BLOCKS // BLK_DEV)
    new_owner_turns = jax.random.permutation(jax.random.fold_in(keys[2], 3), BLOCKS // BLK_DEV)
    new_owner = jax.vmap(lambda own, number: shared_out(jax.random.fold_in(keys[2], 2), own, number, BLK_DEV, N_DP, 1, MOST, 2))(new_owner_keys, new_owner_turns).reshape((BLOCKS, 1))
    code_index = place_ends(jax.random.randint(keys[3], (PARITY_UNITS, N_PARITY), 0, 8), jax.random.fold_in(keys[3], 1), 0, 7).astype(jnp.int32)
    return {"first_moment": first_moment, "second_moment": second_moment, "new_owner": new_owner, "code_index": code_index}


def reference(first_moment, second_moment, new_owner, code_index):
    owner = new_owner.reshape(N_DP, N_PARITY, BLK_DEV).astype(jnp.int32)
    owners = jnp.arange(N_DP, dtype=jnp.int32)
    onehot = (owner[:, :, :, None] == owners[None, None, None, :]).astype(jnp.int32)
    before = (jnp.cumsum(onehot, axis=2).astype(jnp.int32) - onehot).astype(jnp.int32)
    rank = jnp.sum(before * onehot, axis=3).astype(jnp.int32)
    source = jnp.arange(N_DP, dtype=jnp.int32)[:, None, None]
    column = jnp.arange(N_PARITY, dtype=jnp.int32)[None, :, None]
    target = ((owner * N_PARITY + column) * CAP + source * MOST + rank).reshape(-1).astype(jnp.int32)
    new_first = jnp.zeros((N_DP * N_PARITY * CAP, BLOCK), jnp.float32).at[target].set(first_moment)
    new_second = jnp.zeros((N_DP * N_PARITY * CAP, BLOCK), jnp.float32).at[target].set(second_moment)
    loads = jnp.transpose(jnp.sum(onehot, axis=(0, 2)).astype(jnp.int32))
    coef = code_index.astype(jnp.float32) * 0.25
    stacked = jnp.concatenate([new_first, new_second], axis=1).reshape(N_DP, N_PARITY, CAP, 2 * BLOCK)
    parity = jnp.einsum("rp,dpsc->dsrc", coef, stacked, precision=lax.Precision.HIGHEST)
    parity = parity.reshape(N_DP * CAP, PARITY_UNITS * 2 * BLOCK)
    return new_first, new_second, parity, loads
```

```python
import functools

import jax
import jax.numpy as jnp
from jax import lax
from jax.experimental import pallas as pl
from jax.experimental.pallas import tpu as pltpu
from jax.sharding import PartitionSpec as P

MESH = pl.DeviceIdType.MESH


def partner(me, step, n):
    if n & (n - 1):
        return lax.rem(step + n - me, n)
    other, bit = me, 1
    while bit < n:
        if step & bit:
            other = other + bit * (1 - 2 * lax.rem(me // bit, 2))
        bit *= 2
    return other


def kernel(
    n,
    members,
    room,
    slots,
    x_first,
    x_second,
    owner_ref,
    code_ref,
    got_first,
    got_second,
    mixed,
    loads_ref,
    send_first,
    send_second,
    stripe,
    count_send,
    count_got,
    send_sem,
    recv_sem,
    pass_sem,
    land_sem,
    count_send_sem,
    count_recv_sem,
):
    me = lax.axis_index("dp")
    col = lax.axis_index("parity")
    held, width = x_first.shape
    per = n // members
    units = code_ref.shape[0]

    barrier = pltpu.get_barrier_semaphore()
    for step in range(n):
        other = partner(me, step, n)

        @pl.when(other != me)
        def _():
            pl.semaphore_signal(barrier, inc=1, device_id=(other, col), device_id_type=MESH)

    for off in range(1, members):
        pl.semaphore_signal(
            barrier, inc=1, device_id=(me, lax.rem(col + off, members)), device_id_type=MESH
        )

    owner = owner_ref[...]
    names = lax.broadcasted_iota(jnp.int32, (n, held), 0)
    hot = owner == names
    earlier = lax.broadcasted_iota(jnp.int32, (held, held), 0) < lax.broadcasted_iota(
        jnp.int32, (held, held), 1
    )
    before = jnp.dot(
        hot.astype(jnp.bfloat16), earlier.astype(jnp.bfloat16), preferred_element_type=jnp.float32
    )
    rank = jnp.sum(jnp.where(hot, before, 0.0), axis=0, keepdims=True).astype(jnp.int32)
    target = owner * slots + rank
    count = jnp.sum(hot.astype(jnp.int32), axis=1, keepdims=True)
    count_send[...] = jnp.broadcast_to(count, count_send.shape)
    place = (target == lax.broadcasted_iota(jnp.int32, (n * slots, held), 0)).astype(jnp.bfloat16)

    def pack(x_ref, send_ref):
        x = x_ref[...]
        high = x.astype(jnp.bfloat16)
        rest = x - high.astype(jnp.float32)
        mid = rest.astype(jnp.bfloat16)
        low = (rest - mid.astype(jnp.float32)).astype(jnp.bfloat16)
        total = jnp.dot(place, low, preferred_element_type=jnp.float32)
        total += jnp.dot(place, mid, preferred_element_type=jnp.float32)
        total += jnp.dot(place, high, preferred_element_type=jnp.float32)
        send_ref[...] = total

    def rows(index):
        return pl.ds(pl.multiple_of(index * slots, 8), slots)

    sends = ((x_first, send_first, got_first), (x_second, send_second, got_second))

    def exchange(m, step, other):
        return pltpu.make_async_remote_copy(
            src_ref=sends[m][1].at[rows(other)],
            dst_ref=sends[m][2].at[rows(me)],
            send_sem=send_sem.at[m, step],
            recv_sem=recv_sem.at[m, step],
            device_id=(other, col),
            device_id_type=MESH,
        )

    def arrival(m, step, other):
        return pltpu.make_async_remote_copy(
            src_ref=sends[m][1].at[rows(other)],
            dst_ref=sends[m][2].at[rows(other)],
            send_sem=send_sem.at[m, step],
            recv_sem=recv_sem.at[m, step],
            device_id=(other, col),
            device_id_type=MESH,
        )

    def counted(step, other):
        return pltpu.make_async_remote_copy(
            src_ref=count_send,
            dst_ref=count_got.at[step],
            send_sem=count_send_sem.at[step],
            recv_sem=count_recv_sem.at[step],
            device_id=(other, col),
            device_id_type=MESH,
        )

    for m in range(2):
        pack(sends[m][0], sends[m][1])
        if m == 0:
            pl.semaphore_wait(barrier, n - 1 + members - 1)
        for step in range(1, n):
            other = partner(me, step, n)
            exchange(m, step, other).start()
    for step in range(1, n):
        counted(step, partner(me, step, n)).start()

    def onward(m, step, origin, src):
        keeper, place_in = origin // per, lax.rem(origin, per)
        return keeper, pltpu.make_async_remote_copy(
            src_ref=src.at[rows(origin)],
            dst_ref=stripe.at[col, place_in, m],
            send_sem=pass_sem.at[m, step],
            recv_sem=land_sem.at[col, place_in, m],
            device_id=(me, keeper),
            device_id_type=MESH,
        )

    for m in range(2):
        got = sends[m][2]
        got[rows(me), :] = sends[m][1][rows(me), :]

    for m in range(2):
        for step in range(n):
            origin = partner(me, step, n)
            src = sends[m][1] if step == 0 else sends[m][2]
            if step > 0:
                arrival(m, step, origin).wait_recv()
            keeper, copy = onward(m, step, origin, src)

            @pl.when(keeper != col)
            def _():
                copy.start()

    total = count_send[...]
    for step in range(1, n):
        counted(step, partner(me, step, n)).wait_recv()
        total = total + count_got[step]
    mine = lax.broadcasted_iota(jnp.int32, total.shape, 0) == me
    loads_ref[...] = jnp.sum(jnp.where(mine, total, 0), axis=0, keepdims=True)[:, :1]

    for m in range(2):
        for u in range(per):
            origin = col * per + u
            weight = [code_ref[r, col].astype(jnp.float32) * 0.25 for r in range(units)]
            block = sends[m][2][rows(origin), :]
            acc = [block * weight[r] for r in range(units)]
            for off in range(1, members):
                other = lax.rem(col + off, members)
                pltpu.make_async_remote_copy(
                    src_ref=stripe.at[other, u, m],
                    dst_ref=stripe.at[other, u, m],
                    send_sem=pass_sem.at[m, 0],
                    recv_sem=land_sem.at[other, u, m],
                    device_id=(me, other),
                    device_id_type=MESH,
                ).wait_recv()
                block = stripe[other, u, m]
                for r in range(units):
                    acc[r] = acc[r] + block * (code_ref[r, other].astype(jnp.float32) * 0.25)
            for r in range(units):
                mixed[u * slots:(u + 1) * slots, (2 * r + m) * width:(2 * r + m + 1) * width] = acc[r]

    for m in range(2):
        for step in range(n):
            origin = partner(me, step, n)
            src = sends[m][1] if step == 0 else sends[m][2]
            if step > 0:
                exchange(m, step, origin).wait_send()
            keeper, copy = onward(m, step, origin, src)

            @pl.when(keeper != col)
            def _():
                copy.wait_send()
    for step in range(1, n):
        counted(step, partner(me, step, n)).wait_send()


def body(first_moment, second_moment, new_owner, code_index):
    held, width = first_moment.shape
    n = lax.axis_size("dp")
    members = lax.axis_size("parity")
    room = held // n + max(1, held // (4 * n))
    slots = -(-room // 8) * 8
    per = n // members
    units = code_index.shape[0]
    f32 = jnp.float32
    vmem = pl.BlockSpec(memory_space=pltpu.VMEM)
    dma = pltpu.SemaphoreType.DMA
    new_first, new_second, parity, loads = pl.pallas_call(
        functools.partial(kernel, n, members, room, slots),
        out_shape=(
            jax.ShapeDtypeStruct((n * slots, width), f32),
            jax.ShapeDtypeStruct((n * slots, width), f32),
            jax.ShapeDtypeStruct((per * slots, units * 2 * width), f32),
            jax.ShapeDtypeStruct((1, 1), jnp.int32),
        ),
        in_specs=[vmem, vmem, vmem, pl.BlockSpec(memory_space=pltpu.SMEM)],
        out_specs=(vmem, vmem, vmem, vmem),
        scratch_shapes=[
            pltpu.VMEM((n * slots, width), f32),
            pltpu.VMEM((n * slots, width), f32),
            pltpu.VMEM((members, per, 2, slots, width), f32),
            pltpu.VMEM((n, 128), jnp.int32),
            pltpu.VMEM((n, n, 128), jnp.int32),
            dma((2, n)),
            dma((2, n)),
            dma((2, n)),
            dma((members, per, 2)),
            dma((n,)),
            dma((n,)),
        ],
        compiler_params=pltpu.CompilerParams(
            collective_id=0, has_side_effects=True, vmem_limit_bytes=48 * 1024 * 1024
        ),
    )(first_moment, second_moment, new_owner.reshape(1, held), code_index)
    if slots != room:
        new_first, new_second = (
            a.reshape(n, slots, width)[:, :room].reshape(n * room, width)
            for a in (new_first, new_second)
        )
        parity = parity.reshape(per, slots, -1)[:, :room].reshape(per * room, -1)
    return new_first, new_second, parity, loads


def solution(mesh):
    return jax.shard_map(
        body,
        mesh=mesh,
        in_specs=(
            P(("dp", "parity"), None),
            P(("dp", "parity"), None),
            P(("dp", "parity"), None),
            P(),
        ),
        out_specs=(
            P(("dp", "parity"), None),
            P(("dp", "parity"), None),
            P(("dp", "parity"), None),
            P("dp", "parity"),
        ),
        check_vma=False,
    )
```

```python
import functools

import jax
import jax.numpy as jnp
from jax import lax
from jax.experimental import pallas as pl
from jax.experimental.pallas import tpu as pltpu
from jax.sharding import PartitionSpec as P

MESH = pl.DeviceIdType.MESH


def partner(me, step, n):
    if n & (n - 1):
        return lax.rem(step + n - me, n)
    other, bit = me, 1
    while bit < n:
        if step & bit:
            other = other + bit * (1 - 2 * lax.rem(me // bit, 2))
        bit *= 2
    return other


def exchange_kernel(
    n,
    members,
    slots,
    parts,
    first_ref,
    second_ref,
    owner_hbm,
    code_hbm,
    got_first,
    got_second,
    stripe,
    coef_ref,
    loads_ref,
    x_first,
    x_second,
    owner_ref,
    code_ref,
    send_first,
    send_second,
    count_send,
    count_got,
    in_sem,
    send_sem,
    recv_sem,
    pass_sem,
    land_sem,
    count_send_sem,
    count_recv_sem,
):
    me = lax.axis_index("dp")
    col = lax.axis_index("parity")
    held, width = x_first.shape
    per = n // members
    half = n // 2
    size = slots // parts
    units = code_hbm.shape[0]
    moments = ((x_first, send_first, got_first), (x_second, send_second, got_second))

    fetch = [
        pltpu.make_async_copy(src, dst, in_sem.at[i])
        for i, (src, dst) in enumerate(
            (
                (owner_hbm, owner_ref),
                (first_ref, x_first),
                (second_ref, x_second),
                (code_hbm, code_ref),
            )
        )
    ]
    for copy in fetch:
        copy.start()

    barrier = pltpu.get_barrier_semaphore()
    for step in range(1, n):
        pl.semaphore_signal(
            barrier, inc=1, device_id=(partner(me, step, n), col), device_id_type=MESH
        )
    for off in range(1, members):
        pl.semaphore_signal(
            barrier, inc=1, device_id=(me, lax.rem(col + off, members)), device_id_type=MESH
        )

    earlier = (
        lax.broadcasted_iota(jnp.int32, (held, held), 0)
        < lax.broadcasted_iota(jnp.int32, (held, held), 1)
    ).astype(jnp.bfloat16)
    fetch[0].wait()
    owner = owner_ref[...]
    hot = owner == lax.broadcasted_iota(jnp.int32, (n, held), 0)
    before = jnp.dot(hot.astype(jnp.bfloat16), earlier, preferred_element_type=jnp.float32)
    rank = jnp.sum(jnp.where(hot, before, 0.0), axis=0, keepdims=True).astype(jnp.int32)
    target = owner * slots + rank
    side = me // half
    bases = ((1 - side) * half, side * half)

    def pack(m, base, place):
        x = moments[m][0][...]
        high = x.astype(jnp.bfloat16)
        rest = x - high.astype(jnp.float32)
        mid = rest.astype(jnp.bfloat16)
        low = (rest - mid.astype(jnp.float32)).astype(jnp.bfloat16)
        total = jnp.dot(place, low, preferred_element_type=jnp.float32)
        total += jnp.dot(place, mid, preferred_element_type=jnp.float32)
        total += jnp.dot(place, high, preferred_element_type=jnp.float32)
        moments[m][1][pl.ds(pl.multiple_of(base * slots, 8), half * slots), :] = total

    def rows(index, part):
        return pl.ds(pl.multiple_of(index * slots + part * size, 8), size)

    def exchange(m, step, part, source):
        other = partner(me, step, n)
        return pltpu.make_async_remote_copy(
            src_ref=moments[m][1].at[rows(other, part)],
            dst_ref=moments[m][2].at[rows(source, part)],
            send_sem=send_sem.at[m, step, part],
            recv_sem=recv_sem.at[m, step, part],
            device_id=(other, col),
            device_id_type=MESH,
        )

    def counted(step):
        return pltpu.make_async_remote_copy(
            src_ref=count_send,
            dst_ref=count_got.at[step],
            send_sem=count_send_sem.at[step],
            recv_sem=count_recv_sem.at[step],
            device_id=(partner(me, step, n), col),
            device_id_type=MESH,
        )

    def onward(m, step, part):
        origin = partner(me, step, n)
        keeper = origin // per
        return keeper, pltpu.make_async_remote_copy(
            src_ref=moments[m][1 if step == 0 else 2].at[rows(origin, part)],
            dst_ref=stripe.at[m, col, rows(lax.rem(origin, per), part)],
            send_sem=pass_sem.at[m, step, part],
            recv_sem=land_sem.at[m, col, lax.rem(origin, per), part],
            device_id=(me, keeper),
            device_id_type=MESH,
        )

    far, near = range(half, n), range(1, half)
    places = []
    for base in bases:
        spots = lax.broadcasted_iota(jnp.int32, (half * slots, held), 0) + base * slots
        places.append((target == spots).astype(jnp.bfloat16))
    order = ((0, 1), (0, 0), (1, 1), (1, 0))
    for index, (m, side_of) in enumerate(order):
        if m == 0 and index == 0 or m == 1 and all(o[0] == 0 for o in order[:index]):
            fetch[1 + m].wait()
        pack(m, bases[side_of], places[side_of])
        if index == 0:
            pl.semaphore_wait(barrier, n - 1 + members - 1)
        for step in (far, near)[side_of]:
            for part in range(parts):
                exchange(m, step, part, me).start()

    count = jnp.sum(hot.astype(jnp.int32), axis=1, keepdims=True)
    count_send[...] = jnp.broadcast_to(count, count_send.shape)
    own = pl.ds(pl.multiple_of(me * slots, 8), slots)
    for m in range(2):
        moments[m][2][own, :] = moments[m][1][own, :]
    fetch[3].wait()
    for r in range(units):
        for p in range(members):
            coef_ref[r * members + p, :] = jnp.full(
                (128,), code_ref[r, p].astype(jnp.float32) * 0.25, jnp.float32
            )
    for step in range(1, n):
        counted(step).start()

    arrivals = [(m, 0) for m in range(2)]
    for m, side_of in order:
        arrivals += [(m, step) for step in (far, near)[side_of]]
    for m, step in arrivals:
        origin = partner(me, step, n)
        for part in range(parts):
            if step > 0:
                exchange(m, step, part, origin).wait_recv()
            keeper, copy = onward(m, step, part)

            @pl.when(keeper != col)
            def _():
                copy.start()

    for m in range(2):
        kept = pl.ds(pl.multiple_of(col * per * slots, 8), per * slots)
        stripe[m, col] = moments[m][2][kept, :]

    total = count_send[...]
    for step in range(1, n):
        counted(step).wait_recv()
        total = total + count_got[step]
    this = lax.broadcasted_iota(jnp.int32, total.shape, 0) == me
    loads_ref[...] = jnp.sum(jnp.where(this, total, 0), axis=0, keepdims=True)

    for m, step in arrivals:
        for part in range(parts):
            if step > 0:
                exchange(m, step, part, me).wait_send()
            keeper, copy = onward(m, step, part)

            @pl.when(keeper != col)
            def _():
                copy.wait_send()

    for step in range(1, n):
        counted(step).wait_send()

    for m in range(2):
        for off in range(1, members):
            other = lax.rem(col + off, members)
            for u in range(per):
                for part in range(parts):
                    here = stripe.at[m, other, pl.ds(u * slots + part * size, size)]
                    pltpu.make_async_remote_copy(
                        src_ref=here,
                        dst_ref=here,
                        send_sem=pass_sem.at[m, 0, part],
                        recv_sem=land_sem.at[m, other, u, part],
                        device_id=(me, other),
                        device_id_type=MESH,
                    ).wait_recv()


def finish_kernel(
    units,
    members,
    per,
    got_first,
    got_second,
    stripe,
    coef_ref,
    loads_ref,
    out_first,
    out_second,
    out_parity,
    out_loads,
    mixed,
    sem,
):
    width = got_first.shape[1]
    slots = stripe.shape[2] // per
    out = [
        pltpu.make_async_copy(got_first, out_first, sem.at[0]),
        pltpu.make_async_copy(got_second, out_second, sem.at[1]),
    ]
    for copy in out:
        copy.start()
    out_loads[...] = loads_ref[:, :1]
    for u in range(per):
        span = slice(u * slots, (u + 1) * slots)
        for m in range(2):
            for lane in range(width // 128):
                lanes = slice(lane * 128, (lane + 1) * 128)
                blocks = [stripe[m, p, span, lanes] for p in range(members)]
                for r in range(units):
                    acc = blocks[0] * coef_ref[r * members:r * members + 1, :]
                    for p in range(1, members):
                        acc += blocks[p] * coef_ref[r * members + p:r * members + p + 1, :]
                    at = (2 * r + m) * width + lane * 128
                    mixed[span, at:at + 128] = acc
        copy = pltpu.make_async_copy(mixed.at[span], out_parity.at[span], sem.at[2 + u])
        copy.start()
        out.append(copy)
    for copy in out:
        copy.wait()


def body(first_moment, second_moment, new_owner, code_index):
    held, width = first_moment.shape
    n = lax.axis_size("dp")
    members = lax.axis_size("parity")
    room = held // n + max(1, held // (4 * n))
    slots = -(-room // 8) * 8
    parts = 2 if slots % 16 == 0 else 1
    per = n // members
    units = code_index.shape[0]
    f32 = jnp.float32
    hbm = pl.BlockSpec(memory_space=pltpu.HBM)
    vmem = pl.BlockSpec(memory_space=pltpu.VMEM)
    dma = pltpu.SemaphoreType.DMA
    block = jax.ShapeDtypeStruct((n * slots, width), f32)
    got = pl.pallas_call(
        functools.partial(exchange_kernel, n, members, slots, parts),
        out_shape=(
            block,
            block,
            jax.ShapeDtypeStruct((2, members, per * slots, width), f32),
            jax.ShapeDtypeStruct((units * members, 128), f32),
            jax.ShapeDtypeStruct((1, 128), jnp.int32),
        ),
        in_specs=[hbm] * 4,
        out_specs=(vmem,) * 5,
        scratch_shapes=[
            pltpu.VMEM((held, width), f32),
            pltpu.VMEM((held, width), f32),
            pltpu.VMEM((1, held), jnp.int32),
            pltpu.SMEM(code_index.shape, jnp.int32),
            pltpu.VMEM((n * slots, width), f32),
            pltpu.VMEM((n * slots, width), f32),
            pltpu.VMEM((n, 128), jnp.int32),
            pltpu.VMEM((n, n, 128), jnp.int32),
            dma((4,)),
            dma((2, n, parts)),
            dma((2, n, parts)),
            dma((2, n, parts)),
            dma((2, members, per, parts)),
            dma((n,)),
            dma((n,)),
        ],
        compiler_params=pltpu.CompilerParams(
            collective_id=0, has_side_effects=True, vmem_limit_bytes=40 * 1024 * 1024
        ),
    )(first_moment, second_moment, new_owner.reshape(1, held), code_index)
    mixed = (per * slots, units * 2 * width)
    new_first, new_second, parity, loads = pl.pallas_call(
        functools.partial(finish_kernel, units, members, per),
        out_shape=(
            block,
            block,
            jax.ShapeDtypeStruct(mixed, f32),
            jax.ShapeDtypeStruct((1, 1), jnp.int32),
        ),
        in_specs=[vmem] * 5,
        out_specs=(hbm, hbm, hbm, vmem),
        scratch_shapes=[pltpu.VMEM(mixed, f32), dma((2 + per,))],
        compiler_params=pltpu.CompilerParams(vmem_limit_bytes=40 * 1024 * 1024),
    )(*got)
    if slots != room:
        new_first, new_second = (
            a.reshape(n, slots, width)[:, :room].reshape(n * room, width)
            for a in (new_first, new_second)
        )
        parity = parity.reshape(per, slots, -1)[:, :room].reshape(per * room, -1)
    return new_first, new_second, parity, loads


def solution(mesh):
    return jax.shard_map(
        body,
        mesh=mesh,
        in_specs=(
            P(("dp", "parity"), None),
            P(("dp", "parity"), None),
            P(("dp", "parity"), None),
            P(),
        ),
        out_specs=(
            P(("dp", "parity"), None),
            P(("dp", "parity"), None),
            P(("dp", "parity"), None),
            P("dp", "parity"),
        ),
        check_vma=False,
    )
```
